32 devices in a mesh: group: 2 (over x), lat: 16 (over z, y, core).
Axes of the slice: x: 2, y: 2, z: 4, core: 2. Of those that a mesh axis runs over, the one named last changes fastest.
Arguments:
- grid_values: bfloat16 [224, 1440, 256], P(('group', 'lat')), parts along dimension 0, may hold values from -630 to 630
- lat_counts: int32 [16], replicated, may hold values from 1 to 7, 96 in all
- owner_wavenumber: int32 [384], replicated, may hold values from 0 to 383, each once
- legendre: bfloat16 [384, 96, 384], P('lat'), may hold values from -0.625 to 0.625
- quad_weight: float32 [96], replicated, may hold values from 0.3 to 3
- spectral_gain: float32 [384, 256], replicated, may hold values from 0.3 to 3
- channel_mix: bfloat16 [256, 256], replicated, may hold values from -0.375 to 0.375
Outputs:
- grid_output: bfloat16 [224, 1440, 256], P(('group', 'lat')), parts along dimension 0
The draws below stay inside these ranges and needn't reach their ends.
There are 2 independent parts, one for each index of `group`. The reference program is written for one: setup_inputs(seed, part) draws one part's arguments, and reference() takes and returns one part's arrays. A program takes and returns all parts, laid end to end along the dimension named above; an argument that names none is the same for every part. Nothing has to cross between parts.
Inputs may be any that keep to these rules, and one draw needn't show every extreme that they name: `lat_counts`: some device has all 7 slots live. `owner_wavenumber`: each wavenumber appears once; device i of lat owns wavenumber slots i * 24 to (i + 1) * 24 - 1.
All inputs are finite; a program needn't handle non-finite values.
Results may differ from the reference program's by a relative error of at most 0.0095.
Values may be sent and summed in bfloat16 or wider, within the bound.
No kernel may reach another device: no remote copies, remote signals or barrier semaphores. Data moves between devices by JAX's collectives and lax.ppermute only.
A program may use at most 64 MiB of HBM per device.

```python
import math
import jax
import jax.numpy as jnp
import numpy as np
from jax import lax

LONGITUDES = 1440
CHANNELS = 256
WAVES = 384
DEGREES = 384
LAT_SLOTS = 7
SLOTS_ALL = 112
LIVE_LATS = 96
N_LAT = 16


def draw_grid_values(key, part):
    key_rows = jax.random.fold_in(key, 11)
    key_scale = jax.random.fold_in(key, 12)
    key_mean = jax.random.fold_in(key, 13)
    key_noise = jax.random.fold_in(key, 14)
    position = jnp.arange(SLOTS_ALL, dtype=jnp.float32) / SLOTS_ALL
    jitter = jax.random.uniform(key_rows, (SLOTS_ALL,), minval=-0.1, maxval=0.1)
    row_scale = jnp.exp(jnp.log(10.0) * jnp.clip(position + jitter, 0.0, 1.0))
    chan_scale = jnp.exp(jax.random.uniform(key_scale, (CHANNELS,), minval=0.0, maxval=jnp.log(10.0)))
    chan_mean = jax.random.uniform(key_mean, (CHANNELS,), minval=-1.0, maxval=1.0)
    noise = jnp.clip(jax.random.normal(key_noise, (SLOTS_ALL, LONGITUDES, CHANNELS)), -6.0, 6.0)
    values = chan_mean[None, None, :] * chan_scale[None, None, :] + row_scale[:, None, None] * chan_scale[None, None, :] * noise
    return values.astype(jnp.float32).astype(jnp.bfloat16)


def block_levels(rng, shape, cuts, low, top_value):
    loudness, own = 1.0, jax.random.fold_in(rng, 6)
    for dim, blocks in cuts:
        heights = jnp.exp(jax.random.uniform(jax.random.fold_in(own, dim), (blocks,), jnp.float32, low / len(cuts), top_value / len(cuts)))
        loudness = loudness * jnp.repeat(heights, shape[dim] // blocks).reshape([-1 if axis == dim else 1 for axis in range(len(shape))])
    return loudness


def length_profile(number_of, total, reach, lean):
    weights = [(1 << 20) // math.isqrt(rank ** lean) + 1 for rank in range(2, number_of + 1)]
    spare, given = total - reach - (number_of - 1), [1] * (number_of - 1)
    while spare > 0:
        movable = [i for i in range(number_of - 1) if given[i] < reach]
        mass, budget = sum([weights[i] for i in movable]), spare
        for i in movable:
            extra = min(reach - given[i], max(1, budget * weights[i] // mass), spare)
            given[i] = given[i] + extra
            spare = spare - extra
    return np.array([reach] + given)


def ragged(key, amount, total, bound, slope):
    if amount == 2:
        one = jax.random.randint(key, (), max(1, total - bound), min(bound, total - 1) + 1)
        return jnp.stack([one, total - one])
    lengths = jnp.asarray(length_profile(amount, total, bound, slope), jnp.int32)
    pairs = (amount - 1) // 2
    giver, sink = lengths[1:1 + 2 * pairs:2], lengths[2:2 + 2 * pairs:2]
    room = jnp.minimum(giver - 1, bound - sink)
    shifted = jax.random.randint(jax.random.fold_in(key, 1), (pairs,), 0, 1 << 20) % (room + 1)
    lengths = lengths.at[1:1 + 2 * pairs:2].set(giver - shifted).at[2:2 + 2 * pairs:2].set(sink + shifted)
    return lengths[jax.random.permutation(jax.random.fold_in(key, 2), amount)]


def scatter_about(rng, extent, spread, limit, split=(), held_as=jnp.bfloat16):
    level = block_levels(rng, extent, split, -0.22, 0.18) if split else 1.0
    values = jax.random.normal(rng, extent, jnp.float32) * spread * level
    return jnp.minimum(jnp.maximum(values, -limit), limit).astype(held_as)


def setup_inputs(seed: int = 0, part: int = 0) -> dict:
    splits = jax.random.split(jax.random.key(seed), 8)
    own_keys = jax.random.split(jax.random.fold_in(splits[7], part), 8)
    return {
        "grid_values": draw_grid_values(jax.random.fold_in(jax.random.fold_in(splits[7], part), 71), part),
        "lat_counts": ragged(splits[1], N_LAT, LIVE_LATS, LAT_SLOTS, 2).astype(jnp.int32),
        "owner_wavenumber": jax.random.permutation(splits[2], WAVES).astype(jnp.int32),
        "legendre": scatter_about(splits[3], (WAVES, LIVE_LATS, DEGREES), LIVE_LATS ** -0.5, 0.625, ((0, 16),)),
        "quad_weight": jnp.clip(jnp.exp(jax.random.uniform(splits[4], (LIVE_LATS,), jnp.float32, math.log(0.3), math.log(3.0))), 0.3, 3.0),
        "spectral_gain": jnp.clip(jnp.exp(jax.random.uniform(splits[5], (DEGREES, CHANNELS), jnp.float32, math.log(0.3), math.log(3.0))), 0.3, 3.0),
        "channel_mix": scatter_about(splits[6], (CHANNELS, CHANNELS), CHANNELS ** -0.5, 0.375),
    }


def live_slots(lat_counts, slot_count, live_total):
    devices = lat_counts.shape[0]
    starts = jnp.cumsum(lat_counts) - lat_counts
    device_ids = jnp.arange(devices, dtype=jnp.int32)
    slot_ids = jnp.arange(devices * slot_count, dtype=jnp.int32)
    holder = slot_ids // slot_count
    within = slot_ids - holder * slot_count
    holder_hot = holder[:, None] == device_ids[None, :]
    holder_count = lax.optimization_barrier(jnp.sum(jnp.where(holder_hot, lat_counts[None, :], 0), axis=1))
    holder_start = lax.optimization_barrier(jnp.sum(jnp.where(holder_hot, starts[None, :], 0), axis=1))
    slot_valid = within < holder_count
    slot_live = jnp.where(slot_valid, holder_start + within, 0).astype(jnp.int32)
    live_ids = jnp.arange(live_total, dtype=jnp.int32)
    reached = (starts[None, :] <= live_ids[:, None]).astype(jnp.int32)
    source = lax.optimization_barrier(jnp.sum(reached, axis=1)) - 1
    source_hot = source[:, None] == device_ids[None, :]
    source_start = lax.optimization_barrier(jnp.sum(jnp.where(source_hot, starts[None, :], 0), axis=1))
    live_slot = (source * slot_count + live_ids - source_start).astype(jnp.int32)
    return (slot_valid, slot_live, live_slot)

def wave_angles(wave_list, longitudes):
    points = jnp.arange(longitudes, dtype=jnp.int32)
    phase = wave_list[:, None] * points[None, :] % longitudes
    return phase.astype(jnp.float32) * (2.0 * math.pi / longitudes)

def forward_table(wave_list, longitudes):
    angle = wave_angles(wave_list, longitudes)
    factor = 1.0 / math.sqrt(longitudes)
    return jnp.stack([jnp.cos(angle) * factor, -jnp.sin(angle) * factor], axis=1).astype(jnp.bfloat16)

def inverse_table(wave_list, longitudes):
    angle = wave_angles(wave_list, longitudes)
    factor = 1.0 / math.sqrt(longitudes)
    doubled = jnp.where(wave_list > 0, 2.0, 1.0).astype(jnp.float32)[:, None] * factor
    return jnp.stack([jnp.cos(angle) * doubled, -jnp.sin(angle) * doubled], axis=1).astype(jnp.bfloat16)

def reference(grid_values, lat_counts, owner_wavenumber, legendre, quad_weight, spectral_gain, channel_mix):
    slot_valid, slot_live, live_slot = live_slots(lat_counts, LAT_SLOTS, LIVE_LATS)
    row_weight = slot_valid.astype(jnp.float32)[:, None, None]
    widened = grid_values.astype(jnp.float32) * row_weight
    points = LIVE_LATS * LONGITUDES
    channel_mean = lax.optimization_barrier(jnp.sum(widened, axis=(0, 1))) / points
    variance = lax.optimization_barrier(jnp.sum(widened * widened, axis=(0, 1))) / points - channel_mean * channel_mean
    normed = ((grid_values.astype(jnp.float32) - channel_mean) * lax.rsqrt(variance + 1e-05) * row_weight).astype(jnp.bfloat16)
    forward = forward_table(owner_wavenumber, LONGITUDES)
    spectra = jnp.einsum('skc,rtk->srtc', normed.astype(jnp.float32), forward.astype(jnp.float32)).astype(jnp.bfloat16)
    gathered = jnp.take(spectra, live_slot, axis=0)
    weighted = (gathered.astype(jnp.float32) * quad_weight[:, None, None, None]).astype(jnp.bfloat16)
    coefficient = jnp.einsum('rgl,grtc->rltc', legendre.astype(jnp.float32), weighted.astype(jnp.float32))
    degree_mask = (jnp.arange(DEGREES, dtype=jnp.int32)[None, :] >= owner_wavenumber[:, None]).astype(jnp.float32)
    filtered = (coefficient * degree_mask[:, :, None, None] * spectral_gain[None, :, None, :]).astype(jnp.bfloat16)
    mixed = jnp.dot(filtered.reshape(-1, CHANNELS), channel_mix, preferred_element_type=jnp.float32)
    mixed = mixed.astype(jnp.bfloat16).reshape(WAVES, DEGREES, 2, CHANNELS)
    synthesis = jnp.einsum('rgl,rltc->grtc', legendre.astype(jnp.float32), mixed.astype(jnp.float32)).astype(jnp.bfloat16)
    outgoing = jnp.where(slot_valid[:, None, None, None], jnp.take(synthesis, slot_live, axis=0), jnp.zeros((), jnp.bfloat16))
    inverse = inverse_table(owner_wavenumber, LONGITUDES)
    result = jnp.einsum('srtc,rtk->skc', outgoing.astype(jnp.float32), inverse.astype(jnp.float32))
    return result.astype(jnp.bfloat16)
```

```python
import functools
import math

import jax
import jax.numpy as jnp
from jax import lax
from jax.experimental import pallas as pl
from jax.experimental.pallas import tpu as pltpu
from jax.sharding import PartitionSpec as P

F32 = jnp.float32
BF16 = jnp.bfloat16
LANES = 128
PIECES = 6


def split_waves(share):
    first = share // 2
    return (first, share - first)


def slot_maps(lat_counts, slot_count, live_total):
    devices = lat_counts.shape[0]
    ids = jnp.arange(devices, dtype=jnp.int32)
    starts = jnp.sum(jnp.where(ids[None, :] < ids[:, None], lat_counts[None, :], 0), axis=1)
    within = jnp.arange(slot_count, dtype=jnp.int32)
    valid = within[None, :] < lat_counts[:, None]
    live = starts[:, None] + within[None, :]
    lat = jnp.arange(live_total, dtype=jnp.int32)
    hot = valid[:, :, None] & (live[:, :, None] == lat[None, None, :])
    return hot.reshape(devices * slot_count, live_total)


def angle_of(waves, points, longitudes):
    phase = waves * points % longitudes
    return phase.astype(F32) * (2.0 * math.pi / longitudes)


def row_waves(owner_wavenumber, devices, offset, size):
    share = owner_wavenumber.shape[0] // devices
    part = owner_wavenumber.reshape(devices, share)[:, offset : offset + size]
    waves = jnp.broadcast_to(part[:, None, :], (devices, 2, size)).reshape(-1)
    sine = jnp.broadcast_to(
        jnp.arange(2, dtype=jnp.int32)[None, :, None] == 1, (devices, 2, size)
    ).reshape(-1)
    return waves, sine


def forward_parts(waves, sine, longitudes):
    factor = 1.0 / math.sqrt(longitudes)
    tiles = -(-longitudes // LANES)
    low = sine & (waves == 0)
    head = angle_of(waves[:, None], LANES * jnp.arange(tiles, dtype=jnp.int32)[None, :], longitudes)
    step = angle_of(waves[:, None], jnp.arange(LANES, dtype=jnp.int32)[None, :], longitudes)
    use_sine = (sine & (waves != 0))[:, None]
    cos_head, sin_head = jnp.cos(head) * factor, jnp.sin(head) * factor
    head_a = jnp.where(use_sine, -sin_head, cos_head)
    head_b = jnp.where(use_sine, -cos_head, -sin_head)
    return head_a, head_b, jnp.cos(step), jnp.sin(step), low.astype(F32)[:, None]


def inverse_rows(waves, sine, longitudes):
    factor = 1.0 / math.sqrt(longitudes)
    block = next(b for b in (96, 80, 64, 48, 32, 16, 8, 1) if longitudes % b == 0)
    count = longitudes // block
    head = angle_of(waves[None, :], block * jnp.arange(count, dtype=jnp.int32)[:, None], longitudes)
    step = angle_of(waves[None, :], jnp.arange(block, dtype=jnp.int32)[:, None], longitudes)
    cos_head, sin_head = jnp.cos(head) * factor, jnp.sin(head) * factor
    head_a = jnp.where(sine[None, :], -sin_head, cos_head)
    head_b = jnp.where(sine[None, :], -cos_head, -sin_head)
    table = (
        head_a[:, None, :] * jnp.cos(step)[None] + head_b[:, None, :] * jnp.sin(step)[None]
    ).astype(BF16)
    return table.reshape(longitudes, waves.shape[0])


def dft_kernel(
    count_ref, x_ref, head_a, head_b, step_c, step_s, low_ref, out_ref, sum_ref,
    table, stats, *, slots, devices, rows, with_stats,
):
    slot = pl.program_id(0)
    longitudes = x_ref.shape[0]

    @pl.when(slot == 0)
    def _():
        total = jnp.zeros((devices * rows, 1), F32)
        for i in range(head_a.shape[1]):
            width = min(LANES, longitudes - LANES * i)
            piece = (
                head_a[:, i : i + 1] * step_c[:, :width] + head_b[:, i : i + 1] * step_s[:, :width]
            ).astype(BF16)
            table[:, LANES * i : LANES * i + width] = piece
            total += jnp.sum(piece.astype(F32), axis=1, keepdims=True)
        sum_ref[...] = jnp.broadcast_to(total, sum_ref.shape)
        stats[...] = jnp.zeros_like(stats)

    @pl.when(slot < slots)
    def _():
        acc = jnp.dot(table[...], x_ref[...], preferred_element_type=F32)
        acc = acc - low_ref[...] * acc.astype(BF16).astype(F32)
        for d in range(devices):
            out_ref[d] = acc[d * rows : (d + 1) * rows].astype(BF16)

    if with_stats:

        @pl.when(slot < jnp.minimum(count_ref[0], slots))
        def _():
            x = x_ref[...].astype(F32).reshape(longitudes // 8, 8, x_ref.shape[1])
            stats[0] += jnp.sum(x, axis=0)
            stats[1] += jnp.sum(x * x, axis=0)

        @pl.when(slot == slots)
        def _():
            index = lax.broadcasted_iota(jnp.int32, (rows, x_ref.shape[1]), 0)
            block = jnp.zeros((rows, x_ref.shape[1]), F32)
            for k in range(2):
                rest = jnp.sum(stats[k], axis=0, keepdims=True)
                for piece in range(PIECES // 2):
                    part = rest.astype(BF16).astype(F32)
                    block = jnp.where(index == k * (PIECES // 2) + piece, part, block)
                    rest = rest - part
            block = block.astype(BF16)
            for d in range(devices):
                out_ref[d] = block


def dft(grid_values, count, parts, devices, rows, with_stats):
    slots, longitudes, channels = grid_values.shape
    total = devices * rows
    steps = slots + 1 if with_stats else slots
    if with_stats and rows % 8 == 0:
        out_shape = (devices, slots * rows + 8, channels)
        out_spec = pl.BlockSpec((devices, rows, channels), lambda s: (0, s, 0))
    else:
        out_shape = (devices, steps, rows, channels)
        out_spec = pl.BlockSpec((devices, None, rows, channels), lambda s: (0, s, 0, 0))
    whole = lambda a: pl.BlockSpec(a.shape, lambda s: (0,) * a.ndim)
    return pl.pallas_call(
        functools.partial(
            dft_kernel, slots=slots, devices=devices, rows=rows, with_stats=with_stats
        ),
        grid=(steps,),
        in_specs=[
            pl.BlockSpec(memory_space=pltpu.SMEM),
            pl.BlockSpec(
                (None, longitudes, channels), lambda s: (jnp.minimum(s, slots - 1), 0, 0)
            ),
        ]
        + [whole(a) for a in parts],
        out_specs=[out_spec, pl.BlockSpec((total, LANES), lambda s: (0, 0))],
        out_shape=[
            jax.ShapeDtypeStruct(out_shape, BF16),
            jax.ShapeDtypeStruct((total, LANES), F32),
        ],
        scratch_shapes=[
            pltpu.VMEM((total, longitudes), BF16),
            pltpu.VMEM((2, 8, channels), F32),
        ],
        name="dft_stats" if with_stats else "dft",
    )(count, grid_values, *parts)


def mix_kernel(
    wave_ref, sums_ref, raw_ref, leg_ref, hot_ref, weight_ref, moment_ref, gain_ref, mixer_ref,
    out_ref, *, size,
):
    r = pl.program_id(0)
    wave = wave_ref[r]
    leg = jnp.dot(hot_ref[...], leg_ref[...], preferred_element_type=F32).astype(BF16)
    mean, scale = moment_ref[0:1], moment_ref[1:2]
    gain_row = scale * weight_ref[...]
    zero = (wave == 0).astype(F32)
    low = raw_ref[1].astype(F32)
    first = raw_ref[0].astype(F32) + zero * low
    second = low * (1.0 - zero)
    first = (first - mean * sums_ref[r]) * gain_row
    second = (second - mean * (sums_ref[size + r] * (1.0 - zero))) * gain_row
    weighted = jnp.concatenate([first.astype(BF16), second.astype(BF16)], axis=1)
    coefficient = lax.dot_general(
        leg, weighted, (((0,), (0,)), ((), ())), preferred_element_type=F32
    )
    degrees, channels = gain_ref.shape
    degree = lax.broadcasted_iota(jnp.int32, (degrees, channels), 0)
    gain = jnp.where(degree >= wave, gain_ref[...] * (2.0 - zero), 0.0)
    filtered = jnp.concatenate(
        [
            (coefficient[:, :channels] * gain).astype(BF16),
            (coefficient[:, channels:] * gain).astype(BF16),
        ],
        axis=0,
    )
    mixed = jnp.dot(filtered, mixer_ref[...], preferred_element_type=F32).astype(BF16)
    both = jnp.concatenate([mixed[:degrees], mixed[degrees:]], axis=1)
    synthesis = jnp.dot(leg, both, preferred_element_type=F32).astype(BF16)
    out_ref[0] = synthesis[:, :channels]
    out_ref[1] = synthesis[:, channels:]


def mix(raw, waves, sums, legendre, offset, hot, weight, moments, gain, mixer):
    _, size, slots_all, channels = raw.shape
    _, lats, degrees = legendre.shape
    whole = lambda a: pl.BlockSpec(a.shape, lambda r: (0,) * a.ndim)
    smem = pl.BlockSpec(memory_space=pltpu.SMEM)
    block = pl.BlockSpec((2, None, slots_all, channels), lambda r: (0, r, 0, 0))
    return pl.pallas_call(
        functools.partial(mix_kernel, size=size),
        grid=(size,),
        in_specs=[
            smem,
            smem,
            block,
            pl.BlockSpec((None, lats, degrees), lambda r: (r + offset, 0, 0)),
            whole(hot),
            whole(weight),
            whole(moments),
            whole(gain),
            whole(mixer),
        ],
        out_specs=block,
        out_shape=jax.ShapeDtypeStruct(raw.shape, BF16),
        name="mix",
    )(waves, sums, raw, legendre, hot, weight, moments, gain, mixer)


def final_kernel(table_ref, *refs):
    *parts, out_ref, gathered = refs
    at = 0
    for part in parts:
        devices, rows, _ = part.shape
        for d in range(devices):
            gathered[at : at + rows] = part[d]
            at += rows
    out_ref[...] = jnp.dot(
        table_ref[...], gathered[...], preferred_element_type=F32
    ).astype(BF16)


def final(table, parts):
    longitudes, total = table.shape
    devices, slots, _, channels = parts[0].shape
    return pl.pallas_call(
        final_kernel,
        grid=(slots,),
        in_specs=[pl.BlockSpec(table.shape, lambda s: (0, 0))]
        + [
            pl.BlockSpec((devices, None, p.shape[2], channels), lambda s: (0, s, 0, 0))
            for p in parts
        ],
        out_specs=pl.BlockSpec((None, longitudes, channels), lambda s: (s, 0, 0)),
        out_shape=jax.ShapeDtypeStruct((slots, longitudes, channels), BF16),
        scratch_shapes=[pltpu.VMEM((total, channels), BF16)],
        name="inverse",
    )(table, *parts)


def body(
    grid_values, lat_counts, owner_wavenumber, legendre, quad_weight, spectral_gain, channel_mix
):
    slots, longitudes, channels = grid_values.shape
    devices = lat_counts.shape[0]
    share, live_total, _ = legendre.shape
    me = lax.axis_index("lat")
    exchange = lambda a: lax.all_to_all(a, "lat", split_axis=0, concat_axis=0, tiled=True)
    count = lax.dynamic_slice_in_dim(lat_counts, me, 1)
    sizes = split_waves(share)
    offsets = [sum(sizes[:h]) for h in range(len(sizes))]
    rows_of = [
        row_waves(owner_wavenumber, devices, o, n) for o, n in zip(offsets, sizes)
    ]

    received, own_sums = [], []
    for h, size in enumerate(sizes):
        out, sums = dft(
            grid_values, count, forward_parts(*rows_of[h], longitudes), devices, 2 * size, h == 0
        )
        own_sums.append(lax.dynamic_slice(sums, (me * 2 * size, 0), (2 * size, 1))[:, 0])
        received.append(exchange(out))

    hot = slot_maps(lat_counts, slots, live_total)
    weight = jnp.sum(jnp.where(hot, quad_weight[None, :], 0.0), axis=1)[:, None]
    hot = hot.astype(BF16)
    flat = received[0].reshape(devices, -1, channels)
    body_rows = slots * 2 * sizes[0]
    pieces = jnp.sum(
        flat[:, body_rows : body_rows + PIECES].astype(F32).reshape(devices, 2, PIECES // 2, channels),
        axis=2,
    )
    totals = jnp.sum(pieces, axis=0) / (live_total * longitudes)
    variance = totals[1] - totals[0] * totals[0]
    moments = jnp.stack([totals[0], lax.rsqrt(variance + 1e-05)])
    received[0] = flat[:, :body_rows]

    returned = []
    for h, size in enumerate(sizes):
        raw = received[h].reshape(devices * slots, 2, size, channels).transpose(1, 2, 0, 3)
        waves = lax.dynamic_slice_in_dim(owner_wavenumber, me * share + offsets[h], size)
        synthesis = mix(
            raw, waves, own_sums[h], legendre, offsets[h], hot, weight, moments,
            spectral_gain, channel_mix,
        )
        outgoing = synthesis.reshape(2 * size, devices, slots, channels).transpose(1, 2, 0, 3)
        returned.append(exchange(outgoing))

    waves = jnp.concatenate([w for w, _ in rows_of])
    sine = jnp.concatenate([s for _, s in rows_of])
    return final(inverse_rows(waves, sine, longitudes), returned)


def solution(mesh):
    return jax.shard_map(
        body,
        mesh=mesh,
        in_specs=(P(("group", "lat"), None, None), P(), P(), P("lat", None, None), P(), P(), P()),
        out_specs=P(("group", "lat"), None, None),
        check_vma=False,
    )
```

```python
import functools
import math

import jax
import jax.numpy as jnp
from jax import lax
from jax.experimental import pallas as pl
from jax.experimental.pallas import tpu as pltpu
from jax.sharding import PartitionSpec as P

F32 = jnp.float32
BF16 = jnp.bfloat16
LANES = 128
PIECES = 6


def split_waves(share):
    first = share // 2
    return (first, share - first)


def slot_maps(lat_counts, slot_count, live_total):
    devices = lat_counts.shape[0]
    ids = jnp.arange(devices, dtype=jnp.int32)
    starts = jnp.sum(jnp.where(ids[None, :] < ids[:, None], lat_counts[None, :], 0), axis=1)
    within = jnp.arange(slot_count, dtype=jnp.int32)
    valid = within[None, :] < lat_counts[:, None]
    live = starts[:, None] + within[None, :]
    lat = jnp.arange(live_total, dtype=jnp.int32)
    hot = valid[:, :, None] & (live[:, :, None] == lat[None, None, :])
    return hot.reshape(devices * slot_count, live_total)


def angle_of(waves, points, longitudes):
    phase = waves * points % longitudes
    return phase.astype(F32) * (2.0 * math.pi / longitudes)


def row_waves(owner_wavenumber, devices, offset, size):
    share = owner_wavenumber.shape[0] // devices
    part = owner_wavenumber.reshape(devices, share)[:, offset : offset + size]
    waves = jnp.broadcast_to(part[:, None, :], (devices, 2, size)).reshape(-1)
    sine = jnp.broadcast_to(
        jnp.arange(2, dtype=jnp.int32)[None, :, None] == 1, (devices, 2, size)
    ).reshape(-1)
    return waves, sine


def forward_parts(waves, sine, longitudes):
    factor = 1.0 / math.sqrt(longitudes)
    tiles = -(-longitudes // LANES)
    low = sine & (waves == 0)
    head = angle_of(waves[:, None], LANES * jnp.arange(tiles, dtype=jnp.int32)[None, :], longitudes)
    step = angle_of(waves[:, None], jnp.arange(LANES, dtype=jnp.int32)[None, :], longitudes)
    use_sine = (sine & (waves != 0))[:, None]
    cos_head, sin_head = jnp.cos(head) * factor, jnp.sin(head) * factor
    head_a = jnp.where(use_sine, -sin_head, cos_head)
    head_b = jnp.where(use_sine, -cos_head, -sin_head)
    return head_a, head_b, jnp.cos(step), jnp.sin(step), low.astype(F32)[:, None]


def inverse_rows(waves, sine, longitudes):
    factor = 1.0 / math.sqrt(longitudes)
    block = next(b for b in (96, 80, 64, 48, 32, 16, 8, 1) if longitudes % b == 0)
    count = longitudes // block
    head = angle_of(waves[None, :], block * jnp.arange(count, dtype=jnp.int32)[:, None], longitudes)
    step = angle_of(waves[None, :], jnp.arange(block, dtype=jnp.int32)[:, None], longitudes)
    cos_head, sin_head = jnp.cos(head) * factor, jnp.sin(head) * factor
    head_a = jnp.where(sine[None, :], -sin_head, cos_head)
    head_b = jnp.where(sine[None, :], -cos_head, -sin_head)
    table = (
        head_a[:, None, :] * jnp.cos(step)[None] + head_b[:, None, :] * jnp.sin(step)[None]
    ).astype(BF16)
    return table.reshape(longitudes, waves.shape[0])


def dft_kernel(
    count_ref, x_ref, head_a, head_b, step_c, step_s, low_ref, out_ref, sum_ref,
    table, stats, *, slots, devices, rows, with_stats,
):
    slot = pl.program_id(0)
    longitudes = x_ref.shape[0]

    @pl.when(slot == 0)
    def _():
        total = jnp.zeros((devices * rows, 1), F32)
        for i in range(head_a.shape[1]):
            width = min(LANES, longitudes - LANES * i)
            piece = (
                head_a[:, i : i + 1] * step_c[:, :width] + head_b[:, i : i + 1] * step_s[:, :width]
            ).astype(BF16)
            table[:, LANES * i : LANES * i + width] = piece
            total += jnp.sum(piece.astype(F32), axis=1, keepdims=True)
        sum_ref[...] = jnp.broadcast_to(total, sum_ref.shape)
        stats[...] = jnp.zeros_like(stats)

    @pl.when(slot < slots)
    def _():
        acc = jnp.dot(table[...], x_ref[...], preferred_element_type=F32)
        acc = acc - low_ref[...] * acc.astype(BF16).astype(F32)
        for d in range(devices):
            out_ref[d] = acc[d * rows : (d + 1) * rows].astype(BF16)

    if with_stats:

        @pl.when(slot < jnp.minimum(count_ref[lax.axis_index("lat")], slots))
        def _():
            x = x_ref[...].astype(F32).reshape(longitudes // 8, 8, x_ref.shape[1])
            stats[0] += jnp.sum(x, axis=0)
            stats[1] += jnp.sum(x * x, axis=0)

        @pl.when(slot == slots)
        def _():
            index = lax.broadcasted_iota(jnp.int32, (rows, x_ref.shape[1]), 0)
            block = jnp.zeros((rows, x_ref.shape[1]), F32)
            for k in range(2):
                rest = jnp.sum(stats[k], axis=0, keepdims=True)
                for piece in range(PIECES // 2):
                    part = rest.astype(BF16).astype(F32)
                    block = jnp.where(index == k * (PIECES // 2) + piece, part, block)
                    rest = rest - part
            block = block.astype(BF16)
            for d in range(devices):
                out_ref[d] = block


def dft(grid_values, count, parts, devices, rows, with_stats):
    slots, longitudes, channels = grid_values.shape
    total = devices * rows
    steps = slots + 1 if with_stats else slots
    if with_stats and rows % 8 == 0:
        out_shape = (devices, slots * rows + 8, channels)
        out_spec = pl.BlockSpec((devices, rows, channels), lambda s: (0, s, 0))
    else:
        out_shape = (devices, steps, rows, channels)
        out_spec = pl.BlockSpec((devices, None, rows, channels), lambda s: (0, s, 0, 0))
    whole = lambda a: pl.BlockSpec(a.shape, lambda s: (0,) * a.ndim)
    return pl.pallas_call(
        functools.partial(
            dft_kernel, slots=slots, devices=devices, rows=rows, with_stats=with_stats
        ),
        grid=(steps,),
        in_specs=[
            pl.BlockSpec(memory_space=pltpu.SMEM),
            pl.BlockSpec(
                (None, longitudes, channels), lambda s: (jnp.minimum(s, slots - 1), 0, 0)
            ),
        ]
        + [whole(a) for a in parts],
        out_specs=[out_spec, pl.BlockSpec((total, LANES), lambda s: (0, 0))],
        out_shape=[
            jax.ShapeDtypeStruct(out_shape, BF16),
            jax.ShapeDtypeStruct((total, LANES), F32),
        ],
        scratch_shapes=[
            pltpu.VMEM((total, longitudes), BF16),
            pltpu.VMEM((2, 8, channels), F32),
        ],
        name="dft_stats" if with_stats else "dft",
    )(count, grid_values, *parts)


def mix_kernel(
    wave_ref, sums_ref, raw_ref, leg_ref, hot_ref, weight_ref, moment_ref, gain_ref, mixer_ref,
    out_ref, *, size,
):
    r = pl.program_id(0)
    wave = wave_ref[r]
    leg = jnp.dot(hot_ref[...], leg_ref[...], preferred_element_type=F32).astype(BF16)
    mean, scale = moment_ref[0:1], moment_ref[1:2]
    gain_row = scale * weight_ref[...]
    zero = (wave == 0).astype(F32)
    low = raw_ref[1].astype(F32)
    first = raw_ref[0].astype(F32) + zero * low
    second = low * (1.0 - zero)
    first = (first - mean * sums_ref[r]) * gain_row
    second = (second - mean * (sums_ref[size + r] * (1.0 - zero))) * gain_row
    weighted = jnp.concatenate([first.astype(BF16), second.astype(BF16)], axis=1)
    coefficient = lax.dot_general(
        leg, weighted, (((0,), (0,)), ((), ())), preferred_element_type=F32
    )
    degrees, channels = gain_ref.shape
    degree = lax.broadcasted_iota(jnp.int32, (degrees, channels), 0)
    gain = jnp.where(degree >= wave, gain_ref[...] * (2.0 - zero), 0.0)
    filtered = jnp.concatenate(
        [
            (coefficient[:, :channels] * gain).astype(BF16),
            (coefficient[:, channels:] * gain).astype(BF16),
        ],
        axis=0,
    )
    mixed = jnp.dot(filtered, mixer_ref[...], preferred_element_type=F32).astype(BF16)
    both = jnp.concatenate([mixed[:degrees], mixed[degrees:]], axis=1)
    synthesis = jnp.dot(leg, both, preferred_element_type=F32).astype(BF16)
    out_ref[0] = synthesis[:, :channels]
    out_ref[1] = synthesis[:, channels:]


def mix(raw, waves, sums, legendre, offset, hot, weight, moments, gain, mixer):
    _, size, slots_all, channels = raw.shape
    _, lats, degrees = legendre.shape
    whole = lambda a: pl.BlockSpec(a.shape, lambda r: (0,) * a.ndim)
    smem = pl.BlockSpec(memory_space=pltpu.SMEM)
    block = pl.BlockSpec((2, None, slots_all, channels), lambda r: (0, r, 0, 0))
    return pl.pallas_call(
        functools.partial(mix_kernel, size=size),
        grid=(size,),
        in_specs=[
            smem,
            smem,
            block,
            pl.BlockSpec((None, lats, degrees), lambda r: (r + offset, 0, 0)),
            whole(hot),
            whole(weight),
            whole(moments),
            whole(gain),
            whole(mixer),
        ],
        out_specs=block,
        out_shape=jax.ShapeDtypeStruct(raw.shape, BF16),
        name="mix",
    )(waves, sums, raw, legendre, hot, weight, moments, gain, mixer)


def final_kernel(table_ref, *refs):
    *parts, out_ref, gathered = refs
    at = 0
    for part in parts:
        devices, rows, _ = part.shape
        for d in range(devices):
            gathered[at : at + rows] = part[d]
            at += rows
    out_ref[...] = jnp.dot(
        table_ref[...], gathered[...], preferred_element_type=F32
    ).astype(BF16)


def final(table, parts):
    longitudes, total = table.shape
    devices, slots, _, channels = parts[0].shape
    return pl.pallas_call(
        final_kernel,
        grid=(slots,),
        in_specs=[pl.BlockSpec(table.shape, lambda s: (0, 0))]
        + [
            pl.BlockSpec((devices, None, p.shape[2], channels), lambda s: (0, s, 0, 0))
            for p in parts
        ],
        out_specs=pl.BlockSpec((None, longitudes, channels), lambda s: (s, 0, 0)),
        out_shape=jax.ShapeDtypeStruct((slots, longitudes, channels), BF16),
        scratch_shapes=[pltpu.VMEM((total, channels), BF16)],
        name="inverse",
    )(table, *parts)


def body(
    grid_values, lat_counts, owner_wavenumber, legendre, quad_weight, spectral_gain, channel_mix
):
    slots, longitudes, channels = grid_values.shape
    devices = lat_counts.shape[0]
    share, live_total, _ = legendre.shape
    me = lax.axis_index("lat")
    exchange = lambda a: lax.all_to_all(a, "lat", split_axis=0, concat_axis=0, tiled=True)
    sizes = split_waves(share)
    offsets = [sum(sizes[:h]) for h in range(len(sizes))]
    rows_of = [
        row_waves(owner_wavenumber, devices, o, n) for o, n in zip(offsets, sizes)
    ]

    received, own_sums = [], []
    for h, size in enumerate(sizes):
        waves, sine = rows_of[h]
        if h > 0:
            waves, _ = lax.optimization_barrier((waves, sums))
        out, sums = dft(
            grid_values, lat_counts, forward_parts(waves, sine, longitudes), devices, 2 * size,
            h == 0,
        )
        own_sums.append(lax.dynamic_slice(sums, (me * 2 * size, 0), (2 * size, 1))[:, 0])
        received.append(exchange(out))

    hot = slot_maps(lat_counts, slots, live_total)
    weight = jnp.sum(jnp.where(hot, quad_weight[None, :], 0.0), axis=1)[:, None]
    hot = hot.astype(BF16)
    flat = received[0].reshape(devices, -1, channels)
    body_rows = slots * 2 * sizes[0]
    pieces = jnp.sum(
        flat[:, body_rows : body_rows + PIECES].astype(F32).reshape(devices, 2, PIECES // 2, channels),
        axis=2,
    )
    totals = jnp.sum(pieces, axis=0) / (live_total * longitudes)
    variance = totals[1] - totals[0] * totals[0]
    moments = jnp.stack([totals[0], lax.rsqrt(variance + 1e-05)])
    received[0] = flat[:, :body_rows]

    returned = []
    for h, size in enumerate(sizes):
        raw = received[h].reshape(devices * slots, 2, size, channels).transpose(1, 2, 0, 3)
        waves = lax.dynamic_slice_in_dim(owner_wavenumber, me * share + offsets[h], size)
        synthesis = mix(
            raw, waves, own_sums[h], legendre, offsets[h], hot, weight, moments,
            spectral_gain, channel_mix,
        )
        outgoing = synthesis.reshape(2 * size, devices, slots, channels).transpose(1, 2, 0, 3)
        returned.append(exchange(outgoing))

    waves = jnp.concatenate([w for w, _ in rows_of])
    sine = jnp.concatenate([s for _, s in rows_of])
    return final(inverse_rows(waves, sine, longitudes), returned)


def solution(mesh):
    return jax.shard_map(
        body,
        mesh=mesh,
        in_specs=(P(("group", "lat"), None, None), P(), P(), P("lat", None, None), P(), P(), P()),
        out_specs=P(("group", "lat"), None, None),
        check_vma=False,
    )
```

```python
import functools
import math

import jax
import jax.numpy as jnp
from jax import lax
from jax.experimental import pallas as pl
from jax.experimental.pallas import tpu as pltpu
from jax.sharding import PartitionSpec as P

F32 = jnp.float32
BF16 = jnp.bfloat16
LANES = 128
PIECES = 6


def split_waves(share):
    first = share // 2
    return (first, share - first)


def slot_maps(lat_counts, slot_count, live_total):
    devices = lat_counts.shape[0]
    ids = jnp.arange(devices, dtype=jnp.int32)
    starts = jnp.sum(jnp.where(ids[None, :] < ids[:, None], lat_counts[None, :], 0), axis=1)
    within = jnp.arange(slot_count, dtype=jnp.int32)
    valid = within[None, :] < lat_counts[:, None]
    live = starts[:, None] + within[None, :]
    lat = jnp.arange(live_total, dtype=jnp.int32)
    hot = valid[:, :, None] & (live[:, :, None] == lat[None, None, :])
    return hot.reshape(devices * slot_count, live_total)


def angle_of(waves, points, longitudes):
    phase = waves * points % longitudes
    return phase.astype(F32) * (2.0 * math.pi / longitudes)


def row_waves(owner_wavenumber, devices, offset, size):
    share = owner_wavenumber.shape[0] // devices
    part = owner_wavenumber.reshape(devices, share)[:, offset : offset + size]
    waves = jnp.broadcast_to(part[:, None, :], (devices, 2, size)).reshape(-1)
    sine = jnp.broadcast_to(
        jnp.arange(2, dtype=jnp.int32)[None, :, None] == 1, (devices, 2, size)
    ).reshape(-1)
    return waves, sine


def forward_parts(waves, longitudes):
    step = angle_of(waves[:, None], jnp.arange(LANES, dtype=jnp.int32)[None, :], longitudes)
    return jnp.cos(step), jnp.sin(step)


def inverse_rows(waves, sine, longitudes):
    factor = 1.0 / math.sqrt(longitudes)
    block = next(b for b in (96, 80, 64, 48, 32, 16, 8, 1) if longitudes % b == 0)
    count = longitudes // block
    head = angle_of(waves[None, :], block * jnp.arange(count, dtype=jnp.int32)[:, None], longitudes)
    step = angle_of(waves[None, :], jnp.arange(block, dtype=jnp.int32)[:, None], longitudes)
    cos_head, sin_head = jnp.cos(head) * factor, jnp.sin(head) * factor
    head_a = jnp.where(sine[None, :], -sin_head, cos_head)
    head_b = jnp.where(sine[None, :], -cos_head, -sin_head)
    table = (
        head_a[:, None, :] * jnp.cos(step)[None] + head_b[:, None, :] * jnp.sin(step)[None]
    ).astype(BF16)
    return table.reshape(longitudes, waves.shape[0])


def sine_rows(shape, rows):
    row = lax.broadcasted_iota(jnp.int32, shape, 0)
    return lax.rem(row, jnp.int32(rows)) >= rows // 2


def zero_wave(cos_ref, shape):
    return jnp.broadcast_to(cos_ref[:, 1:2], shape) == 1.0


def dft_kernel(
    count_ref, x_ref, cos_ref, sin_ref, out_ref, sum_ref, table, stats,
    *, slots, devices, rows, with_stats,
):
    slot = pl.program_id(0)
    longitudes = x_ref.shape[0]

    @pl.when(slot == 0)
    def _():
        cosine, sine = cos_ref[...], sin_ref[...]
        last = LANES - 1
        turn_c = cosine[:, last:] * cosine[:, 1:2] - sine[:, last:] * sine[:, 1:2]
        turn_s = sine[:, last:] * cosine[:, 1:2] + cosine[:, last:] * sine[:, 1:2]
        turn_c = jnp.broadcast_to(turn_c, cosine.shape)
        turn_s = jnp.broadcast_to(turn_s, cosine.shape)
        factor = 1.0 / math.sqrt(longitudes)
        use_sine = sine_rows(cosine.shape, rows) & jnp.logical_not(zero_wave(cos_ref, cosine.shape))
        own = jnp.where(use_sine, -sine, cosine) * factor
        other = jnp.where(use_sine, cosine, sine) * factor
        total = jnp.zeros(cosine.shape, F32)
        tiles = -(-longitudes // LANES)
        for i in range(tiles):
            width = min(LANES, longitudes - LANES * i)
            piece = own.astype(BF16)
            table[:, LANES * i : LANES * i + width] = piece[:, :width]
            kept = piece.astype(F32)
            if width < LANES:
                lane = lax.broadcasted_iota(jnp.int32, cosine.shape, 1)
                kept = jnp.where(lane < width, kept, 0.0)
            total += kept
            if i + 1 < tiles:
                own, other = own * turn_c - other * turn_s, other * turn_c + own * turn_s
        sum_ref[...] = jnp.broadcast_to(jnp.sum(total, axis=1, keepdims=True), sum_ref.shape)
        stats[...] = jnp.zeros_like(stats)

    @pl.when(slot < slots)
    def _():
        acc = jnp.dot(table[...], x_ref[...], preferred_element_type=F32)
        low = sine_rows(acc.shape, rows) & zero_wave(cos_ref, acc.shape)
        acc = jnp.where(low, acc - acc.astype(BF16).astype(F32), acc)
        for d in range(devices):
            out_ref[d] = acc[d * rows : (d + 1) * rows].astype(BF16)

    if with_stats:

        @pl.when(slot < jnp.minimum(count_ref[lax.axis_index("lat")], slots))
        def _():
            x = x_ref[...].astype(F32).reshape(longitudes // 8, 8, x_ref.shape[1])
            stats[0] += jnp.sum(x, axis=0)
            stats[1] += jnp.sum(x * x, axis=0)

        @pl.when(slot == slots)
        def _():
            index = lax.broadcasted_iota(jnp.int32, (rows, x_ref.shape[1]), 0)
            block = jnp.zeros((rows, x_ref.shape[1]), F32)
            for k in range(2):
                rest = jnp.sum(stats[k], axis=0, keepdims=True)
                for piece in range(PIECES // 2):
                    part = rest.astype(BF16).astype(F32)
                    block = jnp.where(index == k * (PIECES // 2) + piece, part, block)
                    rest = rest - part
            block = block.astype(BF16)
            for d in range(devices):
                out_ref[d] = block


def dft(grid_values, count, parts, devices, rows, with_stats):
    slots, longitudes, channels = grid_values.shape
    total = devices * rows
    steps = slots + 1 if with_stats else slots
    if with_stats and rows % 8 == 0:
        out_shape = (devices, slots * rows + 8, channels)
        out_spec = pl.BlockSpec((devices, rows, channels), lambda s: (0, s, 0))
    else:
        out_shape = (devices, steps, rows, channels)
        out_spec = pl.BlockSpec((devices, None, rows, channels), lambda s: (0, s, 0, 0))
    whole = lambda a: pl.BlockSpec(a.shape, lambda s: (0,) * a.ndim)
    return pl.pallas_call(
        functools.partial(
            dft_kernel, slots=slots, devices=devices, rows=rows, with_stats=with_stats
        ),
        grid=(steps,),
        in_specs=[
            pl.BlockSpec(memory_space=pltpu.SMEM),
            pl.BlockSpec(
                (None, longitudes, channels), lambda s: (jnp.minimum(s, slots - 1), 0, 0)
            ),
        ]
        + [whole(a) for a in parts],
        out_specs=[out_spec, pl.BlockSpec((total, LANES), lambda s: (0, 0))],
        out_shape=[
            jax.ShapeDtypeStruct(out_shape, BF16),
            jax.ShapeDtypeStruct((total, LANES), F32),
        ],
        scratch_shapes=[
            pltpu.VMEM((total, longitudes), BF16),
            pltpu.VMEM((2, 8, channels), F32),
        ],
        name="dft_stats" if with_stats else "dft",
    )(count, grid_values, *parts)


def mix_kernel(
    wave_ref, sums_ref, raw_ref, leg_ref, hot_ref, weight_ref, moment_ref, gain_ref, mixer_ref,
    out_ref, *, size,
):
    r = pl.program_id(0)
    wave = wave_ref[r]
    leg = jnp.dot(hot_ref[...], leg_ref[...], preferred_element_type=F32).astype(BF16)
    mean, scale = moment_ref[0:1], moment_ref[1:2]
    gain_row = scale * weight_ref[...]
    zero = (wave == 0).astype(F32)
    low = raw_ref[1].astype(F32)
    first = raw_ref[0].astype(F32) + zero * low
    second = low * (1.0 - zero)
    first = (first - mean * sums_ref[r]) * gain_row
    second = (second - mean * (sums_ref[size + r] * (1.0 - zero))) * gain_row
    weighted = jnp.concatenate([first.astype(BF16), second.astype(BF16)], axis=1)
    coefficient = lax.dot_general(
        leg, weighted, (((0,), (0,)), ((), ())), preferred_element_type=F32
    )
    degrees, channels = gain_ref.shape
    degree = lax.broadcasted_iota(jnp.int32, (degrees, channels), 0)
    gain = jnp.where(degree >= wave, gain_ref[...] * (2.0 - zero), 0.0)
    filtered = jnp.concatenate(
        [
            (coefficient[:, :channels] * gain).astype(BF16),
            (coefficient[:, channels:] * gain).astype(BF16),
        ],
        axis=0,
    )
    mixed = jnp.dot(filtered, mixer_ref[...], preferred_element_type=F32).astype(BF16)
    both = jnp.concatenate([mixed[:degrees], mixed[degrees:]], axis=1)
    synthesis = jnp.dot(leg, both, preferred_element_type=F32).astype(BF16)
    out_ref[0] = synthesis[:, :channels]
    out_ref[1] = synthesis[:, channels:]


def mix(raw, waves, sums, legendre, offset, hot, weight, moments, gain, mixer):
    _, size, slots_all, channels = raw.shape
    _, lats, degrees = legendre.shape
    whole = lambda a: pl.BlockSpec(a.shape, lambda r: (0,) * a.ndim)
    smem = pl.BlockSpec(memory_space=pltpu.SMEM)
    block = pl.BlockSpec((2, None, slots_all, channels), lambda r: (0, r, 0, 0))
    return pl.pallas_call(
        functools.partial(mix_kernel, size=size),
        grid=(size,),
        in_specs=[
            smem,
            smem,
            block,
            pl.BlockSpec((None, lats, degrees), lambda r: (r + offset, 0, 0)),
            whole(hot),
            whole(weight),
            whole(moments),
            whole(gain),
            whole(mixer),
        ],
        out_specs=block,
        out_shape=jax.ShapeDtypeStruct(raw.shape, BF16),
        name="mix",
    )(waves, sums, raw, legendre, hot, weight, moments, gain, mixer)


def final_kernel(table_ref, *refs):
    *parts, out_ref, gathered = refs
    at = 0
    for part in parts:
        devices, rows, _ = part.shape
        for d in range(devices):
            gathered[at : at + rows] = part[d]
            at += rows
    out_ref[...] = jnp.dot(
        table_ref[...], gathered[...], preferred_element_type=F32
    ).astype(BF16)


def final(table, parts):
    longitudes, total = table.shape
    devices, slots, _, channels = parts[0].shape
    return pl.pallas_call(
        final_kernel,
        grid=(slots,),
        in_specs=[pl.BlockSpec(table.shape, lambda s: (0, 0))]
        + [
            pl.BlockSpec((devices, None, p.shape[2], channels), lambda s: (0, s, 0, 0))
            for p in parts
        ],
        out_specs=pl.BlockSpec((None, longitudes, channels), lambda s: (s, 0, 0)),
        out_shape=jax.ShapeDtypeStruct((slots, longitudes, channels), BF16),
        scratch_shapes=[pltpu.VMEM((total, channels), BF16)],
        name="inverse",
    )(table, *parts)


def body(
    grid_values, lat_counts, owner_wavenumber, legendre, quad_weight, spectral_gain, channel_mix
):
    slots, longitudes, channels = grid_values.shape
    devices = lat_counts.shape[0]
    share, live_total, _ = legendre.shape
    me = lax.axis_index("lat")
    exchange = lambda a: lax.all_to_all(a, "lat", split_axis=0, concat_axis=0, tiled=True)
    sizes = split_waves(share)
    offsets = [sum(sizes[:h]) for h in range(len(sizes))]
    rows_of = [
        row_waves(owner_wavenumber, devices, o, n) for o, n in zip(offsets, sizes)
    ]

    received, own_sums = [], []
    for h, size in enumerate(sizes):
        waves, _ = rows_of[h]
        if h > 0:
            waves, _ = lax.optimization_barrier((waves, sums))
        out, sums = dft(
            grid_values, lat_counts, forward_parts(waves, longitudes), devices, 2 * size,
            h == 0,
        )
        own_sums.append(lax.dynamic_slice(sums, (me * 2 * size, 0), (2 * size, 1))[:, 0])
        received.append(exchange(out))

    hot = slot_maps(lat_counts, slots, live_total)
    weight = jnp.sum(jnp.where(hot, quad_weight[None, :], 0.0), axis=1)[:, None]
    hot = hot.astype(BF16)
    flat = received[0].reshape(devices, -1, channels)
    body_rows = slots * 2 * sizes[0]
    pieces = jnp.sum(
        flat[:, body_rows : body_rows + PIECES].astype(F32).reshape(devices, 2, PIECES // 2, channels),
        axis=2,
    )
    totals = jnp.sum(pieces, axis=0) / (live_total * longitudes)
    variance = totals[1] - totals[0] * totals[0]
    moments = jnp.stack([totals[0], lax.rsqrt(variance + 1e-05)])
    received[0] = flat[:, :body_rows]

    returned = []
    for h, size in enumerate(sizes):
        raw = received[h].reshape(devices * slots, 2, size, channels).transpose(1, 2, 0, 3)
        waves = lax.dynamic_slice_in_dim(owner_wavenumber, me * share + offsets[h], size)
        synthesis = mix(
            raw, waves, own_sums[h], legendre, offsets[h], hot, weight, moments,
            spectral_gain, channel_mix,
        )
        outgoing = synthesis.reshape(2 * size, devices, slots, channels).transpose(1, 2, 0, 3)
        returned.append(exchange(outgoing))

    waves = jnp.concatenate([w for w, _ in rows_of])
    sine = jnp.concatenate([s for _, s in rows_of])
    return final(inverse_rows(waves, sine, longitudes), returned)


def solution(mesh):
    return jax.shard_map(
        body,
        mesh=mesh,
        in_specs=(P(("group", "lat"), None, None), P(), P(), P("lat", None, None), P(), P(), P()),
        out_specs=P(("group", "lat"), None, None),
        check_vma=False,
    )
```

```python
import functools
import math

import jax
import jax.numpy as jnp
from jax import lax
from jax.experimental import pallas as pl
from jax.experimental.pallas import tpu as pltpu
from jax.sharding import PartitionSpec as P

F32 = jnp.float32
BF16 = jnp.bfloat16
LANES = 128
PIECES = 6


def split_waves(share):
    first = share // 2
    return (first, share - first)


def slot_maps(lat_counts, slot_count, live_total):
    devices = lat_counts.shape[0]
    ids = jnp.arange(devices, dtype=jnp.int32)
    starts = jnp.sum(jnp.where(ids[None, :] < ids[:, None], lat_counts[None, :], 0), axis=1)
    within = jnp.arange(slot_count, dtype=jnp.int32)
    valid = within[None, :] < lat_counts[:, None]
    live = starts[:, None] + within[None, :]
    lat = jnp.arange(live_total, dtype=jnp.int32)
    hot = valid[:, :, None] & (live[:, :, None] == lat[None, None, :])
    return hot.reshape(devices * slot_count, live_total)


def angle_of(waves, points, longitudes):
    phase = waves * points % longitudes
    return phase.astype(F32) * (2.0 * math.pi / longitudes)


def row_waves(owner_wavenumber, devices, offset, size):
    share = owner_wavenumber.shape[0] // devices
    part = owner_wavenumber.reshape(devices, share)[:, offset : offset + size]
    waves = jnp.broadcast_to(part[:, None, :], (devices, 2, size)).reshape(-1)
    sine = jnp.broadcast_to(
        jnp.arange(2, dtype=jnp.int32)[None, :, None] == 1, (devices, 2, size)
    ).reshape(-1)
    return waves, sine


def forward_parts(waves, longitudes):
    step = angle_of(waves[:, None], jnp.arange(LANES, dtype=jnp.int32)[None, :], longitudes)
    return jnp.cos(step), jnp.sin(step)


def inverse_rows(waves, sine, longitudes):
    factor = 1.0 / math.sqrt(longitudes)
    block = next(b for b in (96, 80, 64, 48, 32, 16, 8, 1) if longitudes % b == 0)
    count = longitudes // block
    head = angle_of(waves[None, :], block * jnp.arange(count, dtype=jnp.int32)[:, None], longitudes)
    step = angle_of(waves[None, :], jnp.arange(block, dtype=jnp.int32)[:, None], longitudes)
    cos_head, sin_head = jnp.cos(head) * factor, jnp.sin(head) * factor
    head_a = jnp.where(sine[None, :], -sin_head, cos_head)
    head_b = jnp.where(sine[None, :], -cos_head, -sin_head)
    table = (
        head_a[:, None, :] * jnp.cos(step)[None] + head_b[:, None, :] * jnp.sin(step)[None]
    ).astype(BF16)
    return table.reshape(longitudes, waves.shape[0])


def sine_rows(shape, rows):
    row = lax.broadcasted_iota(jnp.int32, shape, 0)
    return lax.rem(row, jnp.int32(rows)) >= rows // 2


def zero_wave(cos_ref, shape):
    return jnp.broadcast_to(cos_ref[:, 1:2], shape) == 1.0


def dft_kernel(
    count_ref, x_ref, cos_ref, sin_ref, out_ref, sum_ref, table, stats,
    *, slots, devices, rows, with_stats,
):
    slot = pl.program_id(0)
    longitudes = x_ref.shape[0]

    @pl.when(slot == 0)
    def _():
        cosine, sine = cos_ref[...], sin_ref[...]
        last = LANES - 1
        turn_c = cosine[:, last:] * cosine[:, 1:2] - sine[:, last:] * sine[:, 1:2]
        turn_s = sine[:, last:] * cosine[:, 1:2] + cosine[:, last:] * sine[:, 1:2]
        turn_c = jnp.broadcast_to(turn_c, cosine.shape)
        turn_s = jnp.broadcast_to(turn_s, cosine.shape)
        factor = 1.0 / math.sqrt(longitudes)
        use_sine = sine_rows(cosine.shape, rows) & jnp.logical_not(zero_wave(cos_ref, cosine.shape))
        own = jnp.where(use_sine, -sine, cosine) * factor
        other = jnp.where(use_sine, cosine, sine) * factor
        total = jnp.zeros(cosine.shape, F32)
        tiles = -(-longitudes // LANES)
        for i in range(tiles):
            width = min(LANES, longitudes - LANES * i)
            piece = own.astype(BF16)
            table[:, LANES * i : LANES * i + width] = piece[:, :width]
            kept = piece.astype(F32)
            if width < LANES:
                lane = lax.broadcasted_iota(jnp.int32, cosine.shape, 1)
                kept = jnp.where(lane < width, kept, 0.0)
            total += kept
            if i + 1 < tiles:
                own, other = own * turn_c - other * turn_s, other * turn_c + own * turn_s
        sum_ref[...] = jnp.broadcast_to(jnp.sum(total, axis=1, keepdims=True), sum_ref.shape)
        stats[...] = jnp.zeros_like(stats)

    @pl.when(slot < slots)
    def _():
        acc = jnp.dot(table[...], x_ref[...], preferred_element_type=F32)
        low = sine_rows(acc.shape, rows) & zero_wave(cos_ref, acc.shape)
        acc = jnp.where(low, acc - acc.astype(BF16).astype(F32), acc)
        for d in range(devices):
            out_ref[d] = acc[d * rows : (d + 1) * rows].astype(BF16)

    if with_stats:

        @pl.when(slot < jnp.minimum(count_ref[lax.axis_index("lat")], slots))
        def _():
            x = x_ref[...].astype(F32).reshape(longitudes // 8, 8, x_ref.shape[1])
            stats[0] += jnp.sum(x, axis=0)
            stats[1] += jnp.sum(x * x, axis=0)

        @pl.when(slot == slots)
        def _():
            index = lax.broadcasted_iota(jnp.int32, (rows, x_ref.shape[1]), 0)
            block = jnp.zeros((rows, x_ref.shape[1]), F32)
            for k in range(2):
                rest = jnp.sum(stats[k], axis=0, keepdims=True)
                for piece in range(PIECES // 2):
                    part = rest.astype(BF16).astype(F32)
                    block = jnp.where(index == k * (PIECES // 2) + piece, part, block)
                    rest = rest - part
            block = block.astype(BF16)
            for d in range(devices):
                out_ref[d] = block


def dft(grid_values, count, parts, devices, rows, with_stats):
    slots, longitudes, channels = grid_values.shape
    total = devices * rows
    steps = slots + 1 if with_stats else slots
    if with_stats and rows % 8 == 0:
        out_shape = (devices, slots * rows + 8, channels)
        out_spec = pl.BlockSpec((devices, rows, channels), lambda s: (0, s, 0))
    else:
        out_shape = (devices, steps, rows, channels)
        out_spec = pl.BlockSpec((devices, None, rows, channels), lambda s: (0, s, 0, 0))
    whole = lambda a: pl.BlockSpec(a.shape, lambda s: (0,) * a.ndim)
    return pl.pallas_call(
        functools.partial(
            dft_kernel, slots=slots, devices=devices, rows=rows, with_stats=with_stats
        ),
        grid=(steps,),
        in_specs=[
            pl.BlockSpec(memory_space=pltpu.SMEM),
            pl.BlockSpec(
                (None, longitudes, channels), lambda s: (jnp.minimum(s, slots - 1), 0, 0)
            ),
        ]
        + [whole(a) for a in parts],
        out_specs=[out_spec, pl.BlockSpec((total, LANES), lambda s: (0, 0))],
        out_shape=[
            jax.ShapeDtypeStruct(out_shape, BF16),
            jax.ShapeDtypeStruct((total, LANES), F32),
        ],
        scratch_shapes=[
            pltpu.VMEM((total, longitudes), BF16),
            pltpu.VMEM((2, 8, channels), F32),
        ],
        name="dft_stats" if with_stats else "dft",
    )(count, grid_values, *parts)


def mix_kernel(
    wave_ref, sums_ref, raw_ref, leg_ref, hot_ref, weight_ref, moment_ref, gain_ref, mixer_ref,
    out_ref, *, size,
):
    r = pl.program_id(0)
    wave = wave_ref[r]
    leg = jnp.dot(hot_ref[...], leg_ref[...], preferred_element_type=F32).astype(BF16)
    mean, scale = moment_ref[0:1], moment_ref[1:2]
    gain_row = scale * weight_ref[...]
    zero = (wave == 0).astype(F32)
    low = raw_ref[1].astype(F32)
    first = raw_ref[0].astype(F32) + zero * low
    second = low * (1.0 - zero)
    first = (first - mean * sums_ref[r]) * gain_row
    second = (second - mean * (sums_ref[size + r] * (1.0 - zero))) * gain_row
    weighted = jnp.concatenate([first.astype(BF16), second.astype(BF16)], axis=1)
    coefficient = lax.dot_general(
        leg, weighted, (((0,), (0,)), ((), ())), preferred_element_type=F32
    )
    degrees, channels = gain_ref.shape
    degree = lax.broadcasted_iota(jnp.int32, (degrees, channels), 0)
    gain = jnp.where(degree >= wave, gain_ref[...] * (2.0 - zero), 0.0)
    filtered = jnp.concatenate(
        [
            (coefficient[:, :channels] * gain).astype(BF16),
            (coefficient[:, channels:] * gain).astype(BF16),
        ],
        axis=0,
    )
    mixed = jnp.dot(filtered, mixer_ref[...], preferred_element_type=F32).astype(BF16)
    both = jnp.concatenate([mixed[:degrees], mixed[degrees:]], axis=1)
    synthesis = jnp.dot(leg, both, preferred_element_type=F32).astype(BF16)
    out_ref[0] = synthesis[:, :channels]
    out_ref[1] = synthesis[:, channels:]


def mix(raw, waves, sums, legendre, offset, hot, weight, moments, gain, mixer):
    _, size, slots_all, channels = raw.shape
    _, lats, degrees = legendre.shape
    whole = lambda a: pl.BlockSpec(a.shape, lambda r: (0,) * a.ndim)
    smem = pl.BlockSpec(memory_space=pltpu.SMEM)
    block = pl.BlockSpec((2, None, slots_all, channels), lambda r: (0, r, 0, 0))
    return pl.pallas_call(
        functools.partial(mix_kernel, size=size),
        grid=(size,),
        in_specs=[
            smem,
            smem,
            block,
            pl.BlockSpec((None, lats, degrees), lambda r: (r + offset, 0, 0)),
            whole(hot),
            whole(weight),
            whole(moments),
            whole(gain),
            whole(mixer),
        ],
        out_specs=block,
        out_shape=jax.ShapeDtypeStruct(raw.shape, BF16),
        name="mix",
    )(waves, sums, raw, legendre, hot, weight, moments, gain, mixer)


def inverse_kernel(table_ref, part_ref, *refs):
    *before, out_ref, gathered = refs
    devices, rows, _ = part_ref.shape
    for d in range(devices):
        gathered[d * rows : (d + 1) * rows] = part_ref[d]
    result = jnp.dot(table_ref[...], gathered[...], preferred_element_type=F32)
    if before:
        result = result + before[0][...].astype(F32)
    out_ref[...] = result.astype(BF16)


def inverse(table, part, before=()):
    longitudes, total = table.shape
    devices, slots, rows, channels = part.shape
    grid_block = pl.BlockSpec((None, longitudes, channels), lambda s: (s, 0, 0))
    return pl.pallas_call(
        inverse_kernel,
        grid=(slots,),
        in_specs=[
            pl.BlockSpec(table.shape, lambda s: (0, 0)),
            pl.BlockSpec((devices, None, rows, channels), lambda s: (0, s, 0, 0)),
        ]
        + [grid_block] * len(before),
        out_specs=grid_block,
        out_shape=jax.ShapeDtypeStruct((slots, longitudes, channels), BF16),
        scratch_shapes=[pltpu.VMEM((total, channels), BF16)],
        name="inverse",
    )(table, part, *before)


def body(
    grid_values, lat_counts, owner_wavenumber, legendre, quad_weight, spectral_gain, channel_mix
):
    slots, longitudes, channels = grid_values.shape
    devices = lat_counts.shape[0]
    share, live_total, _ = legendre.shape
    me = lax.axis_index("lat")
    exchange = lambda a: lax.all_to_all(a, "lat", split_axis=0, concat_axis=0, tiled=True)
    sizes = split_waves(share)
    offsets = [sum(sizes[:h]) for h in range(len(sizes))]
    rows_of = [
        row_waves(owner_wavenumber, devices, o, n) for o, n in zip(offsets, sizes)
    ]

    received, own_sums = [], []
    for h, size in enumerate(sizes):
        waves, _ = rows_of[h]
        if h > 0:
            waves, _ = lax.optimization_barrier((waves, sums))
        out, sums = dft(
            grid_values, lat_counts, forward_parts(waves, longitudes), devices, 2 * size,
            h == 0,
        )
        own_sums.append(lax.dynamic_slice(sums, (me * 2 * size, 0), (2 * size, 1))[:, 0])
        received.append(exchange(out))

    hot = slot_maps(lat_counts, slots, live_total)
    weight = jnp.sum(jnp.where(hot, quad_weight[None, :], 0.0), axis=1)[:, None]
    hot = hot.astype(BF16)
    flat = received[0].reshape(devices, -1, channels)
    body_rows = slots * 2 * sizes[0]
    pieces = jnp.sum(
        flat[:, body_rows : body_rows + PIECES].astype(F32).reshape(devices, 2, PIECES // 2, channels),
        axis=2,
    )
    totals = jnp.sum(pieces, axis=0) / (live_total * longitudes)
    variance = totals[1] - totals[0] * totals[0]
    moments = jnp.stack([totals[0], lax.rsqrt(variance + 1e-05)])
    received[0] = flat[:, :body_rows]

    returned = []
    for h, size in enumerate(sizes):
        raw = received[h].reshape(devices * slots, 2, size, channels).transpose(1, 2, 0, 3)
        waves = lax.dynamic_slice_in_dim(owner_wavenumber, me * share + offsets[h], size)
        synthesis = mix(
            raw, waves, own_sums[h], legendre, offsets[h], hot, weight, moments,
            spectral_gain, channel_mix,
        )
        outgoing = synthesis.reshape(2 * size, devices, slots, channels).transpose(1, 2, 0, 3)
        returned.append(exchange(outgoing))

    result = ()
    for (waves, sine), part in zip(rows_of, returned):
        result = (inverse(inverse_rows(waves, sine, longitudes), part, result),)
    return result[0]


def solution(mesh):
    return jax.shard_map(
        body,
        mesh=mesh,
        in_specs=(P(("group", "lat"), None, None), P(), P(), P("lat", None, None), P(), P(), P()),
        out_specs=P(("group", "lat"), None, None),
        check_vma=False,
    )
```
